32 devices in a mesh: rep: 4 (over x, y), dp: 8 (over z, core).
Axes of the slice: x: 2, y: 2, z: 4, core: 2. Of those that a mesh axis runs over, the one named last changes fastest.
Arguments:
- a: bfloat16 [32, 4, 8192, 1280], P(('rep', 'dp')), parts along dimension 0
- g: bfloat16 [32, 4, 8192, 3072], P(('rep', 'dp')), parts along dimension 0
Outputs:
- output: bfloat16 [16, 1280, 3072], P('rep'), parts along dimension 0
There are 4 independent parts. The reference program is written for one: setup_inputs(seed, part) draws one part's arguments, and reference() takes and returns one part's arrays. A program takes and returns all parts, laid end to end along the dimension named above; each array names one.
All inputs are finite; a program needn't handle non-finite values.
Results may differ from the reference program's by a relative error of at most 0.012.
Values are sent between devices in bfloat16 or wider.
A program may use at most 2 GiB of HBM per device.

```python
import jax
import jax.numpy as jnp
from jax import lax

DEVICES = 8
MATRICES = 4
TOKENS = 8192
D = 1280
FF = 3072


def setup_inputs(seed: int = 0, part: int = 0) -> dict:
    ka, kg, ks = (jax.random.fold_in(k, part) for k in jax.random.split(jax.random.key(seed), 3))
    size = 2.0 ** jax.random.uniform(ks, (DEVICES, MATRICES, 1, 1), jnp.float32, -1.0, 1.0)
    a = jax.random.normal(ka, (DEVICES, MATRICES, TOKENS, D), jnp.float32)
    g = size * jax.random.normal(kg, (DEVICES, MATRICES, TOKENS, FF), jnp.float32) * (DEVICES * TOKENS) ** -0.5
    return {"a": a.astype(jnp.bfloat16), "g": g.astype(jnp.bfloat16)}


def reference(a, g):
    def take(so_far, one):
        return so_far + jnp.einsum("ntd,ntf->ndf", *one, preferred_element_type=jnp.float32), None

    return lax.scan(take, jnp.zeros((MATRICES, D, FF), jnp.float32), (a, g))[0].astype(jnp.bfloat16)
```

```python
import functools

import jax
import jax.numpy as jnp
from jax import lax
from jax.experimental import pallas as pl
from jax.experimental.pallas import tpu as pltpu
from jax.sharding import PartitionSpec as P

MESH = pl.DeviceIdType.MESH
BM, BN = 640, 256
HALF, CH = BM // 2, BM // 4
ND, NP, NS, NT, NG, NF = 3, 8, 6, 4, 3, 4
DX, D1, D2, D3, D4 = 1, 3, 5, 7, 9


def kernel(dims, a, g, out, abuf, gbuf, acc, pend, dout, din, lsend, lrecv, psend, precv, tbuf,
           asem, gsem, d_s, d_r, l_s, l_r, p_s, p_r, t_sp, t_sl, t_sd, t_st, f_sl, f_sd, pt_r, lt_r, dt_r,
           cr_d, cr_l, cr_p):
    nm, K, M, N = dims
    I, J = M // BM, N // BN
    total = nm * I * J
    rep, dp = lax.axis_index("rep"), lax.axis_index("dp")
    z, c = dp // 2, lax.rem(dp, 2)
    sd = z // 2
    leaf = (z == 0) | (z == 3)
    inner = jnp.logical_not(leaf)
    rq, sq = sd, 1 - sd
    mate = (rep, z * 2 + 1 - c)
    near = (rep, jnp.where(leaf, 1 + sd, 3 * sd) * 2 + c)
    peer = (rep, (2 - sd) * 2 + c)

    bar = pltpu.get_barrier_semaphore()
    pl.semaphore_signal(bar, inc=1, device_id=mate, device_id_type=MESH)
    pl.semaphore_signal(bar, inc=1, device_id=near, device_id_type=MESH)

    @pl.when(inner)
    def _():
        pl.semaphore_signal(bar, inc=1, device_id=peer, device_id_type=MESH)

    def acopy(q, slot):
        n, i = q // I, lax.rem(q, I)
        return pltpu.make_async_copy(a.at[n, :, pl.ds(pl.multiple_of(i * BM, 128), BM)], abuf.at[slot], asem.at[slot])

    def gcopy(p, slot):
        n, j = p // (I * J), lax.rem(p, J)
        return pltpu.make_async_copy(g.at[n, :, pl.ds(pl.multiple_of(j * BN, 128), BN)], gbuf.at[slot], gsem.at[slot])

    acopy(0, 0).start()
    for p in range(NG - 1):
        gcopy(p, p).start()

    @pl.when(leaf)
    def _():
        pl.semaphore_wait(bar, 2)

    @pl.when(inner)
    def _():
        pl.semaphore_wait(bar, 3)

    def place(p, core, q):
        n, i, j = p // (I * J), lax.rem(p // J, I), lax.rem(p, J)
        row = i * BM + core * HALF + q * CH
        return out.at[n, pl.ds(pl.multiple_of(row, 32), CH), pl.ds(pl.multiple_of(j * BN, 128), BN)]

    def remote(src, dst, s, r, who):
        return pltpu.make_async_remote_copy(src, dst, s, r, device_id=who, device_id_type=MESH)

    def d_copy(p):
        return remote(dout.at[lax.rem(p, 2)], din.at[lax.rem(p, ND)], d_s.at[lax.rem(p, 2)], d_r.at[lax.rem(p, ND)], mate)

    def l_copy(p, q):
        s = lax.rem(p, NS)
        return remote(lsend.at[s, q], lrecv.at[s, q], l_s.at[s, q], l_r.at[s, q], near)

    def p_copy(p):
        s = lax.rem(p, NS)
        return remote(psend.at[s], precv.at[s], p_s.at[s], p_r.at[s], peer)

    def t_peer(p, q):
        s = lax.rem(p, NT)
        return remote(tbuf.at[s], place(p, c, q), t_sp.at[s], pt_r.at[p], peer)

    def t_leaf(p, q):
        s = lax.rem(p, NT)
        return remote(tbuf.at[s], place(p, c, q), t_sl.at[s], lt_r.at[p, 0], near)

    def t_mate(p, q):
        s = lax.rem(p, NT)
        return remote(tbuf.at[s], place(p, c, q), t_sd.at[s], dt_r.at[p, 0], mate)

    def t_own(p, q):
        s = lax.rem(p, NT)
        return pltpu.make_async_copy(tbuf.at[s], place(p, c, q), t_st.at[s])

    def f_leaf(p, q):
        return remote(place(p, c, q), place(p, c, q), f_sl.at[lax.rem(p, NF)], lt_r.at[p, 1], near)

    def f_mate(p, q, k):
        return remote(place(p, c, q), place(p, c, q), f_sd.at[lax.rem(p, NF), k], dt_r.at[p, k], mate)

    f32, bf16 = jnp.float32, jnp.bfloat16

    def compute(p):
        q = p // J
        qs, s = lax.rem(q, 2), lax.rem(p, NG)

        @pl.when(p + NG - 1 < total)
        def _():
            gcopy(p + NG - 1, lax.rem(p + NG - 1, NG)).start()

        @pl.when(lax.rem(p, J) == 0)
        def _():
            acopy(q, qs).wait()

            @pl.when(q + 1 < nm * I)
            def _():
                acopy(q + 1, 1 - qs).start()

        gcopy(p, s).wait()
        acc[...] = lax.dot_general(abuf[qs], gbuf[s], (((0,), (0,)), ((), ())), preferred_element_type=f32)

        @pl.when(p >= 2)
        def _():
            d_copy(p - 2).wait_send()

        ds, ps = lax.rem(p, 2), lax.rem(p, NP)
        for k in range(2):
            dout[ds, k] = acc[pl.ds(pl.multiple_of((1 - c) * HALF + k * CH, 32), CH), :].astype(bf16)

        @pl.when(p >= ND)
        def _():
            pl.semaphore_wait(cr_d, 1)

        d_copy(p).start()
        for k in range(2):
            pend[ps, k] = acc[pl.ds(pl.multiple_of(c * HALF + k * CH, 32), CH), :]

    def chip_sum(p):
        d_copy(p).wait_recv()
        ps, ds, ls = lax.rem(p, NP), lax.rem(p, ND), lax.rem(p, NS)

        @pl.when(leaf)
        def _():
            @pl.when(p >= NS)
            def _():
                pl.semaphore_wait(cr_l, 1)

            for q in (sq, rq):
                @pl.when(p >= NS)
                def _():
                    l_copy(p - NS, q).wait_send()

                lsend[ls, q] = (pend[ps, q] + din[ds, q].astype(f32)).astype(bf16)
                l_copy(p, q).start()

        @pl.when(inner)
        def _():
            for k in range(2):
                pend[ps, k] = pend[ps, k] + din[ds, k].astype(f32)

        @pl.when(p + ND < total)
        def _():
            pl.semaphore_signal(cr_d, inc=1, device_id=mate, device_id_type=MESH)

    def forward_partial(p):
        ps, s = lax.rem(p, NP), lax.rem(p, NS)
        l_copy(p, sq).wait_recv()

        @pl.when(p >= NS)
        def _():
            p_copy(p - NS).wait_send()
            pl.semaphore_wait(cr_p, 1)

        psend[s] = (pend[ps, sq] + lrecv[s, sq].astype(f32)).astype(bf16)
        p_copy(p).start()

    def finish(p):
        ps, s, t = lax.rem(p, NP), lax.rem(p, NS), lax.rem(p, NT)
        l_copy(p, rq).wait_recv()
        p_copy(p).wait_recv()

        @pl.when(p >= NT)
        def _():
            for f in (t_peer, t_leaf, t_mate):
                f(p - NT, rq).wait_send()
            t_own(p - NT, rq).wait()

        tbuf[t] = (pend[ps, rq] + lrecv[s, rq].astype(f32) + precv[s].astype(f32)).astype(bf16)
        t_peer(p, rq).start()
        t_leaf(p, rq).start()
        t_mate(p, rq).start()
        t_own(p, rq).start()

        @pl.when(p + NS < total)
        def _():
            pl.semaphore_signal(cr_l, inc=1, device_id=near, device_id_type=MESH)
            pl.semaphore_signal(cr_p, inc=1, device_id=peer, device_id_type=MESH)

    def pass_on(p):
        t_peer(p, sq).wait_recv()

        @pl.when(p >= NF)
        def _():
            f_leaf(p - NF, sq).wait_send()
            f_mate(p - NF, sq, 1).wait_send()

        f_leaf(p, sq).start()
        f_mate(p, sq, 1).start()

    def pass_leaf(p):
        t_leaf(p, rq).wait_recv()

        @pl.when(p >= NF)
        def _():
            f_mate(p - NF, rq, 0).wait_send()
            f_mate(p - NF, sq, 1).wait_send()

        f_mate(p, rq, 0).start()
        f_leaf(p, sq).wait_recv()
        f_mate(p, sq, 1).start()

    def within(e):
        return (e >= 0) & (e < total)

    def events(s):
        @pl.when(within(s - DX))
        def _():
            chip_sum(s - DX)

        @pl.when(inner)
        def _():
            @pl.when(within(s - D1))
            def _():
                forward_partial(s - D1)

            @pl.when(within(s - D2))
            def _():
                finish(s - D2)

            @pl.when(within(s - D3))
            def _():
                pass_on(s - D3)

        @pl.when(leaf & within(s - D4))
        def _():
            pass_leaf(s - D4)

    def step(s, _):
        compute(s)
        events(s)
        return 0

    lax.fori_loop(0, total, step, 0)

    def tail(s, _):
        events(s)
        return 0

    lax.fori_loop(total, total + max(D3, D4), tail, 0)

    for p in range(total - 2, total):
        d_copy(p).wait_send()

    def gone(lo, f):
        def body(p, _):
            f(p)
            return 0
        lax.fori_loop(lo, total, body, 0)

    @pl.when(leaf)
    def _():
        def f(p):
            l_copy(p, sq).wait_send()
            l_copy(p, rq).wait_send()
        gone(total - NS, f)

        def f(p):
            f_mate(p, rq, 0).wait_send()
            f_mate(p, sq, 1).wait_send()
        gone(total - NF, f)

    @pl.when(inner)
    def _():
        gone(total - NS, lambda p: p_copy(p).wait_send())

        def f(p):
            t_peer(p, rq).wait_send()
            t_leaf(p, rq).wait_send()
            t_mate(p, rq).wait_send()
            t_own(p, rq).wait()
        gone(total - NT, f)

        def f(p):
            f_leaf(p, sq).wait_send()
            f_mate(p, sq, 1).wait_send()
        gone(total - NF, f)

    def arrived(p):
        for k, q in ((0, rq), (1, sq)):
            where = place(p, 1 - c, q)
            remote(where, where, f_sd.at[0, 0], dt_r.at[p, k], mate).wait_recv()
    gone(0, arrived)


def solution(mesh):
    def step(a, g):
        _, nm, K, M = a.shape
        N = g.shape[-1]
        a, g = a.reshape(nm, K, M), g.reshape(nm, K, N)
        total = nm * (M // BM) * (N // BN)
        dma = pltpu.SemaphoreType.DMA
        bf16, f32 = jnp.bfloat16, jnp.float32
        return pl.pallas_call(
            functools.partial(kernel, (nm, K, M, N)),
            out_shape=jax.ShapeDtypeStruct((nm, M, N), bf16),
            in_specs=[pl.BlockSpec(memory_space=pl.ANY)] * 2,
            out_specs=pl.BlockSpec(memory_space=pl.ANY),
            scratch_shapes=[
                pltpu.VMEM((2, K, BM), bf16),
                pltpu.VMEM((NG, K, BN), bf16),
                pltpu.VMEM((BM, BN), f32),
                pltpu.VMEM((NP, 2, CH, BN), f32),
                pltpu.VMEM((2, 2, CH, BN), bf16),
                pltpu.VMEM((ND, 2, CH, BN), bf16),
                pltpu.VMEM((NS, 2, CH, BN), bf16),
                pltpu.VMEM((NS, 2, CH, BN), bf16),
                pltpu.VMEM((NS, CH, BN), bf16),
                pltpu.VMEM((NS, CH, BN), bf16),
                pltpu.VMEM((NT, CH, BN), bf16),
                dma((2,)), dma((NG,)), dma((2,)), dma((ND,)), dma((NS, 2)), dma((NS, 2)), dma((NS,)), dma((NS,)),
                dma((NT,)), dma((NT,)), dma((NT,)), dma((NT,)), dma((NF,)), dma((NF, 2)),
                dma((total,)), dma((total, 2)), dma((total, 2)),
                pltpu.SemaphoreType.REGULAR, pltpu.SemaphoreType.REGULAR, pltpu.SemaphoreType.REGULAR,
            ],
            compiler_params=pltpu.CompilerParams(
                collective_id=0, has_side_effects=True, vmem_limit_bytes=62 * 2**20
            ),
        )(a, g)

    return jax.shard_map(
        step,
        mesh=mesh,
        in_specs=(P(("rep", "dp"), None, None, None),) * 2,
        out_specs=P("rep", None, None),
        check_vma=False,
    )
```

```python
import functools

import jax
import jax.numpy as jnp
from jax import lax
from jax.experimental import pallas as pl
from jax.experimental.pallas import tpu as pltpu
from jax.sharding import PartitionSpec as P

MESH = pl.DeviceIdType.MESH
BM, BN, KS = 640, 512, 4
U = 2
HALF, CH, CW = BM // 2, BM // 8, 2 * BN // U
WC = BN // CW
ND, NP, NS, NQ, NF = 2, 4, 4, 8, 8
RP, RL, RM = 8, 12, 7
OX, O1, O2, O3, O4, O5 = 1, 6, 9, 12, 18, 24
PUT = 4


def kernel(dims, a, g, out, abuf, gbuf, acc, pend, dout, din, lsend, lrecv, psend, precv,
           asem, gsem, d_s, d_r, l_s, l_r, p_s, p_r, t_sp, t_sl, f_sl, m_s, pt_r, lt_r, m_r,
           cr_d, cr_l, cr_p):
    nm, K, M, N = dims
    I, J, KC = M // BM, N // BN, K // KS
    total = nm * I * J
    units = U * total
    rep, dp = lax.axis_index("rep"), lax.axis_index("dp")
    z, c = dp // 2, lax.rem(dp, 2)
    sd = z // 2
    leaf = (z == 0) | (z == 3)
    inner = jnp.logical_not(leaf)
    rq, sq = sd, 1 - sd
    mate = (rep, z * 2 + 1 - c)
    near = (rep, jnp.where(leaf, 1 + sd, 3 * sd) * 2 + c)
    peer = (rep, (2 - sd) * 2 + c)
    f32, bf16 = jnp.float32, jnp.bfloat16

    bar = pltpu.get_barrier_semaphore()
    pl.semaphore_signal(bar, inc=1, device_id=mate, device_id_type=MESH)
    pl.semaphore_signal(bar, inc=1, device_id=near, device_id_type=MESH)

    @pl.when(inner)
    def _():
        pl.semaphore_signal(bar, inc=1, device_id=peer, device_id_type=MESH)

    def acopy(q, k):
        n, i = q // I, lax.rem(q, I)
        return pltpu.make_async_copy(
            a.at[n, pl.ds(k * KC, KC), pl.ds(pl.multiple_of(i * BM, 128), BM)], abuf.at[k], asem.at[k])

    def gcopy(p, k):
        n, j = p // (I * J), lax.rem(p, J)
        return pltpu.make_async_copy(
            g.at[n, pl.ds(k * KC, KC), pl.ds(pl.multiple_of(j * BN, 128), BN)], gbuf.at[k], gsem.at[k])

    for k in range(KS):
        acopy(0, k).start()
        gcopy(0, k).start()

    def start(p):
        n, i, j = p // (I * J), lax.rem(p // J, I), lax.rem(p, J)
        return n, i * BM, j * BN

    def place(u, q):
        n, row, col = start(u // U)
        row += c * HALF + (2 * q + lax.rem(u, U) // WC) * CH
        if WC > 1:
            col += lax.rem(u, WC) * CW
        return out.at[n, pl.ds(pl.multiple_of(row, 16), CH), pl.ds(pl.multiple_of(col, 128), CW)]

    def block(p, core, q):
        n, row, col = start(p)
        row += core * HALF + 2 * q * CH
        return out.at[n, pl.ds(pl.multiple_of(row, 16), 2 * CH), pl.ds(pl.multiple_of(col, 128), BN)]

    def remote(src, dst, s, r, who):
        return pltpu.make_async_remote_copy(src, dst, s, r, device_id=who, device_id_type=MESH)

    def d_copy(p):
        s = lax.rem(p, ND)
        return remote(dout.at[s], din.at[s], d_s.at[s], d_r.at[s], mate)

    def l_copy(u, q):
        s, h = lax.rem(u // U, NS), lax.rem(u, U)
        return remote(lsend.at[s, h, q], lrecv.at[s, h, q], l_s.at[s, h, q], l_r.at[s, h, q], near)

    def p_copy(u):
        s = lax.rem(u, NQ)
        return remote(psend.at[s], precv.at[s], p_s.at[s], p_r.at[s], peer)

    def t_peer(u, q):
        return remote(place(u, q), place(u, q), t_sp.at[lax.rem(u, NF)], pt_r.at[lax.rem(u, RP)], peer)

    def t_leaf(u, q):
        return remote(place(u, q), place(u, q), t_sl.at[lax.rem(u, NF)], lt_r.at[lax.rem(u, RL), 0], near)

    def f_leaf(u, q):
        return remote(place(u, q), place(u, q), f_sl.at[lax.rem(u, NF)], lt_r.at[lax.rem(u, RL), 1], near)

    def m_copy(p, q):
        return remote(block(p, c, q), block(p, c, q), m_s.at[lax.rem(p, 2), q], m_r.at[lax.rem(p, RM), q], mate)

    def to_mate(p, q):
        @pl.when(p >= 2)
        def _():
            m_copy(p - 2, q).wait_send()

        m_copy(p, q).start()

    def multiply(p, k):
        q, j = p // J, lax.rem(p, J)

        @pl.when(j == 0)
        def _():
            acopy(q, k).wait()

        gcopy(p, k).wait()
        d = lax.dot_general(abuf[k], gbuf[k], (((0,), (0,)), ((), ())), preferred_element_type=f32)
        if k == 0:
            acc[...] = d
        else:
            acc[...] += d

        @pl.when(p + 1 < total)
        def _():
            gcopy(p + 1, k).start()

            @pl.when(j == J - 1)
            def _():
                acopy(q + 1, k).start()

    def swap(p):
        s, ps = lax.rem(p, ND), lax.rem(p, NP)

        @pl.when(p >= ND)
        def _():
            d_copy(p - ND).wait_send()
            pl.semaphore_wait(cr_d, 1)

        def part(core, h, q):
            rows = pl.ds(pl.multiple_of(core * HALF + (2 * q + h // WC) * CH, 16), CH)
            cols = slice(h % WC * CW, (h % WC + 1) * CW)
            return acc[rows, cols]

        for h in range(U):
            for q in range(2):
                dout[s, h, q] = part(1 - c, h, q).astype(bf16)
        d_copy(p).start()
        for h in range(U):
            for q in range(2):
                pend[ps, h, q] = part(c, h, q)

    def chip_sum(p):
        d_copy(p).wait_recv()
        ps, ds, ls = lax.rem(p, NP), lax.rem(p, ND), lax.rem(p, NS)

        @pl.when(leaf)
        def _():
            @pl.when(p >= NS)
            def _():
                pl.semaphore_wait(cr_l, 1)

            for h in range(U):
                for q in (sq, rq):
                    @pl.when(p >= NS)
                    def _():
                        l_copy(U * (p - NS) + h, q).wait_send()

                    lsend[ls, h, q] = (pend[ps, h, q] + din[ds, h, q].astype(f32)).astype(bf16)
                    l_copy(U * p + h, q).start()

        @pl.when(inner)
        def _():
            for h in range(U):
                for q in range(2):
                    pend[ps, h, q] = pend[ps, h, q] + din[ds, h, q].astype(f32)

        @pl.when(p + ND < total)
        def _():
            pl.semaphore_signal(cr_d, inc=1, device_id=mate, device_id_type=MESH)

    def forward_partial(u):
        p, h, s = u // U, lax.rem(u, U), lax.rem(u, NQ)
        l_copy(u, sq).wait_recv()

        @pl.when(u >= NQ)
        def _():
            p_copy(u - NQ).wait_send()
            pl.semaphore_wait(cr_p, 1)

        psend[s] = (pend[lax.rem(p, NP), h, sq] + lrecv[lax.rem(p, NS), h, sq].astype(f32)).astype(bf16)
        p_copy(u).start()

    def finish(u):
        p, h, s = u // U, lax.rem(u, U), lax.rem(u, NQ)
        l_copy(u, rq).wait_recv()
        p_copy(u).wait_recv()

        @pl.when(u >= NF)
        def _():
            t_peer(u - NF, rq).wait_send()
            t_leaf(u - NF, rq).wait_send()

        where = place(u, rq)
        where[...] = (pend[lax.rem(p, NP), h, rq] + lrecv[lax.rem(p, NS), h, rq].astype(f32)
                      + precv[s].astype(f32)).astype(bf16)
        t_leaf(u, rq).start()
        t_peer(u, rq).start()

        @pl.when(u + NQ < units)
        def _():
            pl.semaphore_signal(cr_p, inc=1, device_id=peer, device_id_type=MESH)

        @pl.when(h == U - 1)
        def _():
            to_mate(p, rq)

            @pl.when(p + NS < total)
            def _():
                pl.semaphore_signal(cr_l, inc=1, device_id=near, device_id_type=MESH)

    def pass_on(u):
        t_peer(u, sq).wait_recv()

        @pl.when(u >= NF)
        def _():
            f_leaf(u - NF, sq).wait_send()

        f_leaf(u, sq).start()

        @pl.when(lax.rem(u, U) == U - 1)
        def _():
            to_mate(u // U, sq)

    def pass_leaf(u):
        t_leaf(u, rq).wait_recv()

        @pl.when(lax.rem(u, U) == U - 1)
        def _():
            to_mate(u // U, rq)

        f_leaf(u, sq).wait_recv()

        @pl.when(lax.rem(u, U) == U - 1)
        def _():
            to_mate(u // U, sq)

    def arrived(p):
        for q in range(2):
            where = block(p, 1 - c, q)
            remote(where, where, m_s.at[0, 0], m_r.at[lax.rem(p, RM), q], mate).wait_recv()

    def events(p, k):
        def due(lag, per, f):
            t = k - lag
            if t % per == 0:
                e = (4 // per) * p + t // per

                @pl.when((e >= 0) & (e < (4 // per) * total))
                def _():
                    f(e)

        due(3 + OX, 4, chip_sum)
        due(3 + O5, 4, arrived)

        @pl.when(inner)
        def _():
            due(O1, 4 // U, forward_partial)
            due(O2, 4 // U, finish)
            due(O3, 4 // U, pass_on)

        @pl.when(leaf)
        def _():
            due(O4, 4 // U, pass_leaf)

    def step(p, _):
        for k in range(KS):
            multiply(p, k)
            if k == 0:
                @pl.when(p == 0)
                def _():
                    pl.semaphore_wait(bar, jnp.where(leaf, 2, 3))
            if k == KS - 1:
                swap(p)
            events(p, k)
        return 0

    lax.fori_loop(0, total, step, 0)

    def tail(p, _):
        for k in range(KS):
            events(p, k)
        return 0

    lax.fori_loop(total, total + (O5 + 3) // 4 + 1, tail, 0)

    def gone(lo, hi, f):
        def body(p, _):
            f(p)
            return 0
        lax.fori_loop(lo, hi, body, 0)

    gone(total - ND, total, lambda p: d_copy(p).wait_send())

    def f(p):
        m_copy(p, rq).wait_send()
        m_copy(p, sq).wait_send()
    gone(total - 2, total, f)

    @pl.when(leaf)
    def _():
        def f(u):
            l_copy(u, sq).wait_send()
            l_copy(u, rq).wait_send()
        gone(units - U * NS, units, f)

    @pl.when(inner)
    def _():
        gone(units - NQ, units, lambda u: p_copy(u).wait_send())

        def f(u):
            t_peer(u, rq).wait_send()
            t_leaf(u, rq).wait_send()
            f_leaf(u, sq).wait_send()
        gone(units - NF, units, f)


def put(x, out, sems):
    rows = x.shape[1] // PUT
    copies = [
        pltpu.make_async_copy(x.at[n, pl.ds(r * rows, rows)], out.at[n, pl.ds(r * rows, rows)], sems.at[n, r])
        for n in range(x.shape[0]) for r in range(PUT)
    ]
    for one in copies:
        one.start()
    for one in copies:
        one.wait()


def solution(mesh):
    def step(a, g):
        _, nm, K, M = a.shape
        N = g.shape[-1]
        a, g = a.reshape(nm, K, M), g.reshape(nm, K, N)
        total = nm * (M // BM) * (N // BN)
        dma = pltpu.SemaphoreType.DMA
        bf16, f32 = jnp.bfloat16, jnp.float32
        sums = pl.pallas_call(
            functools.partial(kernel, (nm, K, M, N)),
            out_shape=pltpu.VMEM((nm, M, N), bf16),
            in_specs=[pl.BlockSpec(memory_space=pl.ANY)] * 2,
            out_specs=pl.BlockSpec(memory_space=pltpu.VMEM),
            scratch_shapes=[
                pltpu.VMEM((KS, K // KS, BM), bf16),
                pltpu.VMEM((KS, K // KS, BN), bf16),
                pltpu.VMEM((BM, BN), f32),
                pltpu.VMEM((NP, U, 2, CH, CW), f32),
                pltpu.VMEM((ND, U, 2, CH, CW), bf16),
                pltpu.VMEM((ND, U, 2, CH, CW), bf16),
                pltpu.VMEM((NS, U, 2, CH, CW), bf16),
                pltpu.VMEM((NS, U, 2, CH, CW), bf16),
                pltpu.VMEM((NQ, CH, CW), bf16),
                pltpu.VMEM((NQ, CH, CW), bf16),
                dma((KS,)), dma((KS,)), dma((ND,)), dma((ND,)), dma((NS, U, 2)), dma((NS, U, 2)),
                dma((NQ,)), dma((NQ,)), dma((NF,)), dma((NF,)), dma((NF,)), dma((2, 2)),
                dma((RP,)), dma((RL, 2)), dma((RM, 2)),
                pltpu.SemaphoreType.REGULAR, pltpu.SemaphoreType.REGULAR, pltpu.SemaphoreType.REGULAR,
            ],
            compiler_params=pltpu.CompilerParams(
                collective_id=0, has_side_effects=True, vmem_limit_bytes=33 * 2**20
            ),
        )(a, g)
        return pl.pallas_call(
            put,
            out_shape=jax.ShapeDtypeStruct((nm, M, N), bf16),
            in_specs=[pl.BlockSpec(memory_space=pltpu.VMEM)],
            out_specs=pl.BlockSpec(memory_space=pl.ANY),
            scratch_shapes=[dma((nm, PUT))],
            compiler_params=pltpu.CompilerParams(vmem_limit_bytes=2**20),
        )(sums)

    return jax.shard_map(
        step,
        mesh=mesh,
        in_specs=(P(("rep", "dp"), None, None, None),) * 2,
        out_specs=P("rep", None, None),
        check_vma=False,
    )
```

```python
import functools

import jax
import jax.numpy as jnp
from jax import lax
from jax.experimental import pallas as pl
from jax.experimental.pallas import tpu as pltpu
from jax.sharding import PartitionSpec as P

MESH = pl.DeviceIdType.MESH
BM, BN, KS = 640, 512, 4
U = 2
HALF, CH, CW = BM // 2, BM // 8, 2 * BN // U
WC = BN // CW
ND, NP, NS, NR, NF = 2, 4, 4, 2, 2
RP, RL, RM = 3, 4, 7
SUM, HELD = 4, 25
PARTIAL = 5, 5
FINISH = 9, 6
PASS = 10, 11
LEAF = 19
HEAD = 10
PUT = 4


def kernel(dims, a, g, out, abuf, gbuf, acc, pend, dout, din, lsend, lrecv, psend, precv,
           asem, gsem, d_s, d_r, l_s, l_r, p_s, p_r, t_sp, t_sl, f_sl, m_s, pt_r, lt_r, m_r,
           cr_d, cr_l, cr_p):
    nm, K, M, N = dims
    I, J, KC = M // BM, N // BN, K // KS
    total = nm * I * J
    rep, dp = lax.axis_index("rep"), lax.axis_index("dp")
    z, c = lax.div(dp, 2), lax.rem(dp, 2)
    sd = lax.div(z, 2)
    leaf = (z == 0) | (z == 3)
    inner = jnp.logical_not(leaf)
    rq, sq = sd, 1 - sd
    mate = (rep, z * 2 + 1 - c)
    near = (rep, jnp.where(leaf, 1 + sd, 3 * sd) * 2 + c)
    peer = (rep, (2 - sd) * 2 + c)
    f32, bf16 = jnp.float32, jnp.bfloat16

    bar = pltpu.get_barrier_semaphore()
    pl.semaphore_signal(bar, inc=1, device_id=mate, device_id_type=MESH)
    pl.semaphore_signal(bar, inc=1, device_id=near, device_id_type=MESH)

    @pl.when(inner)
    def _():
        pl.semaphore_signal(bar, inc=1, device_id=peer, device_id_type=MESH)

    def start(p):
        n, i, j = lax.div(p, I * J), lax.rem(lax.div(p, J), I), lax.rem(p, J)
        return n, i * BM, j * BN

    def acopy(q, k):
        n, i = lax.div(q, I), lax.rem(q, I)
        return pltpu.make_async_copy(
            a.at[n, pl.ds(k * KC, KC), pl.ds(pl.multiple_of(i * BM, 128), BM)], abuf.at[k], asem.at[k])

    def gcopy(p, k):
        n, _, col = start(p)
        return pltpu.make_async_copy(
            g.at[n, pl.ds(k * KC, KC), pl.ds(pl.multiple_of(col, 128), BN)], gbuf.at[k], gsem.at[k])

    for k in range(KS):
        acopy(0, k).start()
        gcopy(0, k).start()

    def remote(src, dst, s, r, who):
        return pltpu.make_async_remote_copy(src, dst, s, r, device_id=who, device_id_type=MESH)

    class Piece:
        def __init__(self, p, sure, place=None):
            self.p, self.sure, self.place = p, sure, place or start(p)

        def slot(self, n):
            return lax.rem(self.p, n)

        def half(self, core):
            n, row, col = self.place
            row = row + core * HALF
            return out.at[n, pl.ds(pl.multiple_of(row, 16), HALF), pl.ds(pl.multiple_of(col, 128), BN)]

        def block(self, core, q):
            n, row, col = self.place
            row = row + core * HALF + 2 * q * CH
            return out.at[n, pl.ds(pl.multiple_of(row, 16), 2 * CH), pl.ds(pl.multiple_of(col, 128), BN)]

        def message(self, q, h):
            n, row, col = self.place
            row, col = row + c * HALF + (2 * q + h // WC) * CH, col + h % WC * CW
            return out.at[n, pl.ds(pl.multiple_of(row, 16), CH), pl.ds(pl.multiple_of(col, 128), CW)]

        def d_copy(self):
            s = self.slot(ND)
            return remote(dout.at[s], din.at[s], d_s.at[s], d_r.at[s], mate)

        def l_copy(self, h, q):
            s = self.slot(NS)
            return remote(lsend.at[s, h, q], lrecv.at[s, h, q], l_s.at[s], l_r.at[s, h, q], near)

        def p_copy(self, h):
            s = self.slot(NR)
            return remote(psend.at[s, h], precv.at[s, h], p_s.at[s], p_r.at[s, h], peer)

        def t_peer(self, h, q):
            at = self.message(q, h)
            return remote(at, at, t_sp.at[self.slot(NF)], pt_r.at[self.slot(RP), h], peer)

        def t_leaf(self, h, q):
            at = self.message(q, h)
            return remote(at, at, t_sl.at[self.slot(NF)], lt_r.at[self.slot(RL)], near)

        def f_leaf(self, h, q):
            at = self.message(q, h)
            return remote(at, at, f_sl.at[self.slot(NF)], lt_r.at[self.slot(RL)], near)

        def m_copy(self, q):
            at = self.block(c, q)
            return remote(at, at, m_s.at[self.slot(2)], m_r.at[self.slot(RM)], mate)

        def l_sent(self):
            s = self.slot(NS)
            remote(lsend.at[s], lrecv.at[s], l_s.at[s], l_r.at[s, 0, 0], near).wait_send()

        def p_sent(self):
            s = self.slot(NR)
            remote(psend.at[s], precv.at[s], p_s.at[s], p_r.at[s, 0], peer).wait_send()

        def t_sent(self):
            s, at = self.slot(NF), self.block(c, rq)
            remote(at, at, t_sp.at[s], pt_r.at[0, 0], peer).wait_send()
            remote(at, at, t_sl.at[s], lt_r.at[0], near).wait_send()

        def f_sent(self):
            at = self.block(c, sq)
            remote(at, at, f_sl.at[self.slot(NF)], lt_r.at[0], near).wait_send()

        def m_sent(self):
            at = self.half(c)
            remote(at, at, m_s.at[self.slot(2)], m_r.at[0], mate).wait_send()

        def whole(self):
            at = self.half(c)
            remote(at, at, t_sl.at[0], lt_r.at[self.slot(RL)], near).wait_recv()

        def given(self):
            at = self.half(1 - c)
            remote(at, at, m_s.at[0], m_r.at[self.slot(RM)], mate).wait_recv()

    def multiply(p, k):
        q, j = lax.div(p, J), lax.rem(p, J)

        @pl.when(j == 0)
        def _():
            acopy(q, k).wait()

        gcopy(p, k).wait()
        d = lax.dot_general(abuf[k], gbuf[k], (((0,), (0,)), ((), ())), preferred_element_type=f32)
        if k == 0:
            acc[...] = d
        else:
            acc[...] += d

        @pl.when(p + 1 < total)
        def _():
            gcopy(p + 1, k).start()

            @pl.when(j == J - 1)
            def _():
                acopy(q + 1, k).start()

    def again(it, n, f):
        if it.sure:
            f()
        else:
            pl.when(it.p >= n)(f)

    def swap(it):
        s, ps = it.slot(ND), it.slot(NP)

        def free():
            it.d_copy().wait_send()
            pl.semaphore_wait(cr_d, 1)
        again(it, ND, free)

        def part(core, h, q):
            rows = pl.ds(pl.multiple_of(core * HALF + (2 * q + h // WC) * CH, 16), CH)
            return acc[rows, h % WC * CW:(h % WC + 1) * CW]

        for h in range(U):
            for q in range(2):
                dout[s, h, q] = part(1 - c, h, q).astype(bf16)
        it.d_copy().start()
        for h in range(U):
            for q in range(2):
                pend[ps, h, q] = part(c, h, q)

    def chip_sum(it):
        it.d_copy().wait_recv()
        ps, ds, ls = it.slot(NP), it.slot(ND), it.slot(NS)

        @pl.when(leaf)
        def _():
            def free():
                pl.semaphore_wait(cr_l, 1)
                it.l_sent()
            again(it, NS, free)
            for h in range(U):
                for q in (sq, rq):
                    lsend[ls, h, q] = (pend[ps, h, q] + din[ds, h, q].astype(f32)).astype(bf16)
                    it.l_copy(h, q).start()

        @pl.when(inner)
        def _():
            for h in range(U):
                for q in range(2):
                    pend[ps, h, q] = pend[ps, h, q] + din[ds, h, q].astype(f32)

        pl.semaphore_signal(cr_d, inc=1, device_id=mate, device_id_type=MESH)

    def forward_partial(it, h):
        it.l_copy(h, sq).wait_recv()
        if h == 0:
            again(it, NR, it.p_sent)
        again(it, NR, lambda: pl.semaphore_wait(cr_p, 1))
        psend[it.slot(NR), h] = (pend[it.slot(NP), h, sq] + lrecv[it.slot(NS), h, sq].astype(f32)).astype(bf16)
        it.p_copy(h).start()

    def finish(it, h):
        it.l_copy(h, rq).wait_recv()
        it.p_copy(h).wait_recv()
        if h == 0:
            again(it, NF, it.t_sent)
        where = it.message(rq, h)
        where[...] = (pend[it.slot(NP), h, rq] + lrecv[it.slot(NS), h, rq].astype(f32)
                      + precv[it.slot(NR), h].astype(f32)).astype(bf16)
        it.t_leaf(h, rq).start()
        it.t_peer(h, rq).start()
        pl.semaphore_signal(cr_p, inc=1, device_id=peer, device_id_type=MESH)
        if h == U - 1:
            again(it, 2, it.m_sent)
            it.m_copy(rq).start()
            pl.semaphore_signal(cr_l, inc=1, device_id=near, device_id_type=MESH)

    def pass_on(it, h):
        it.t_peer(h, sq).wait_recv()
        if h == 0:
            again(it, NF, it.f_sent)
        it.f_leaf(h, sq).start()
        if h == U - 1:
            it.m_copy(sq).start()

    def pass_leaf(it):
        it.whole()
        again(it, 2, it.m_sent)
        it.m_copy(rq).start()
        it.m_copy(sq).start()

    def arrived(it):
        it.given()

    def events(pieces, k, phase):
        def due(lag, f, *h):
            if (k - lag) % 4:
                return
            it = pieces[(lag - k) // 4]
            if phase == "body":
                f(it, *h)
            else:
                pl.when(it.p >= 0 if phase == "head" else it.p < total)(lambda: f(it, *h))

        def inners(side):
            for lags, f in ((PARTIAL, forward_partial), (FINISH, finish), (PASS, pass_on)):
                for h in range(U):
                    due(lags[side] + 4 // U * h, f, h)

        for side in range(2):
            pl.when(inner & (sd == side))(functools.partial(inners, side))
        due(SUM, chip_sum)

        @pl.when(leaf)
        def _():
            due(LEAF, pass_leaf)

        due(HELD, arrived)

    def recent(p, phase):
        return [Piece(p - n, phase != "head") for n in range(HELD // 4 + 1)]

    def step(phase, p, _):
        pieces = recent(p, phase)
        for k in range(KS):
            multiply(p, k)
            if k == 0 and phase == "head":
                @pl.when(p == 0)
                def _():
                    pl.semaphore_wait(bar, jnp.where(leaf, 2, 3))
            if k == KS - 1:
                swap(pieces[0])
            events(pieces, k, phase)
        return 0

    lax.fori_loop(0, HEAD, functools.partial(step, "head"), 0)
    lax.fori_loop(HEAD, total, functools.partial(step, "body"), 0)

    def tail(p, _):
        pieces = recent(p, "tail")
        for k in range(KS):
            events(pieces, k, "tail")
        return 0

    last = total + HELD // 4 + 1
    lax.fori_loop(total, last - 2, tail, 0)

    def gone(n, f):
        def body(p, _):
            f(Piece(p, True))
            return 0
        lax.fori_loop(total - n, total, body, 0)

    pl.semaphore_wait(cr_d, ND)
    gone(ND, lambda it: it.d_copy().wait_send())

    @pl.when(leaf)
    def _():
        pl.semaphore_wait(cr_l, NS)
        gone(NS, Piece.l_sent)

    @pl.when(inner)
    def _():
        pl.semaphore_wait(cr_p, NR * U)
        gone(NR, Piece.p_sent)
        gone(NF, Piece.t_sent)
        gone(NF, Piece.f_sent)

    lax.fori_loop(last - 2, last, tail, 0)

    gone(2, Piece.m_sent)


def put(x, out, sems):
    rows = x.shape[1] // PUT
    copies = [
        pltpu.make_async_copy(x.at[n, pl.ds(r * rows, rows)], out.at[n, pl.ds(r * rows, rows)], sems.at[n, r])
        for n in range(x.shape[0]) for r in range(PUT)
    ]
    for one in copies:
        one.start()
    for one in copies:
        one.wait()


def solution(mesh):
    def step(a, g):
        _, nm, K, M = a.shape
        N = g.shape[-1]
        a, g = a.reshape(nm, K, M), g.reshape(nm, K, N)
        dma = pltpu.SemaphoreType.DMA
        bf16, f32 = jnp.bfloat16, jnp.float32
        sums = pl.pallas_call(
            functools.partial(kernel, (nm, K, M, N)),
            out_shape=pltpu.VMEM((nm, M, N), bf16),
            in_specs=[pl.BlockSpec(memory_space=pl.ANY)] * 2,
            out_specs=pl.BlockSpec(memory_space=pltpu.VMEM),
            scratch_shapes=[
                pltpu.VMEM((KS, K // KS, BM), bf16),
                pltpu.VMEM((KS, K // KS, BN), bf16),
                pltpu.VMEM((BM, BN), f32),
                pltpu.VMEM((NP, U, 2, CH, CW), f32),
                pltpu.VMEM((ND, U, 2, CH, CW), bf16),
                pltpu.VMEM((ND, U, 2, CH, CW), bf16),
                pltpu.VMEM((NS, U, 2, CH, CW), bf16),
                pltpu.VMEM((NS, U, 2, CH, CW), bf16),
                pltpu.VMEM((NR, U, CH, CW), bf16),
                pltpu.VMEM((NR, U, CH, CW), bf16),
                dma((KS,)), dma((KS,)), dma((ND,)), dma((ND,)), dma((NS,)), dma((NS, U, 2)),
                dma((NR,)), dma((NR, U)), dma((NF,)), dma((NF,)), dma((NF,)), dma((2,)),
                dma((RP, U)), dma((RL,)), dma((RM,)),
                pltpu.SemaphoreType.REGULAR, pltpu.SemaphoreType.REGULAR, pltpu.SemaphoreType.REGULAR,
            ],
            compiler_params=pltpu.CompilerParams(
                collective_id=0, has_side_effects=True, vmem_limit_bytes=33 * 2**20
            ),
        )(a, g)
        return pl.pallas_call(
            put,
            out_shape=jax.ShapeDtypeStruct((nm, M, N), bf16),
            in_specs=[pl.BlockSpec(memory_space=pltpu.VMEM)],
            out_specs=pl.BlockSpec(memory_space=pl.ANY),
            scratch_shapes=[dma((nm, PUT))],
            compiler_params=pltpu.CompilerParams(vmem_limit_bytes=2**20),
        )(sums)

    return jax.shard_map(
        step,
        mesh=mesh,
        in_specs=(P(("rep", "dp"), None, None, None),) * 2,
        out_specs=P("rep", None, None),
        check_vma=False,
    )
```

```python
import functools

import jax
import jax.numpy as jnp
from jax import lax
from jax.experimental import pallas as pl
from jax.experimental.pallas import tpu as pltpu
from jax.sharding import PartitionSpec as P

MESH = pl.DeviceIdType.MESH
BM, BN, KS = 640, 512, 4
FIRST = 2
U = 2
HALF, CH, CW = BM // 2, BM // 8, 2 * BN // U
WC = BN // CW
ND, NP, NS, NR, NF = 2, 4, 4, 2, 2
RP, RL, RM = 3, 4, 7
SUM, HELD = 4, 25
PARTIAL = 5, 5
FINISH = 9, 6
PASS = 10, 11
LEAF = 19
HEAD = 10
PUT = 4


def div(x, n):
    return x // n if isinstance(x, int) else lax.div(x, n)


def rem(x, n):
    return x % n if isinstance(x, int) else lax.rem(x, n)


def whole_of(x, n):
    return x if isinstance(x, int) else pl.multiple_of(x, n)


def kernel(dims, a, g, out, abuf, gbuf, acc, pend, dout, din, lsend, lrecv, psend, precv,
           asem, gsem, d_s, d_r, l_s, l_r, p_s, p_r, t_sp, t_sl, f_sl, m_s, pt_r, lt_r, m_r,
           cr_d, cr_l, cr_p):
    nm, K, M, N = dims
    I, J, KC = M // BM, N // BN, K // KS
    total = nm * I * J
    rep, dp = lax.axis_index("rep"), lax.axis_index("dp")
    z, c = lax.div(dp, 2), lax.rem(dp, 2)
    sd = lax.div(z, 2)
    leaf = (z == 0) | (z == 3)
    inner = jnp.logical_not(leaf)
    rq, sq = sd, 1 - sd
    mate = (rep, z * 2 + 1 - c)
    near = (rep, jnp.where(leaf, 1 + sd, 3 * sd) * 2 + c)
    peer = (rep, (2 - sd) * 2 + c)
    f32, bf16 = jnp.float32, jnp.bfloat16

    bar = pltpu.get_barrier_semaphore()
    pl.semaphore_signal(bar, inc=1, device_id=mate, device_id_type=MESH)
    pl.semaphore_signal(bar, inc=1, device_id=near, device_id_type=MESH)

    @pl.when(inner)
    def _():
        pl.semaphore_signal(bar, inc=1, device_id=peer, device_id_type=MESH)

    def start(p):
        n, i, j = div(p, I * J), rem(div(p, J), I), rem(p, J)
        return n, i * BM, j * BN

    def acopy(q, k):
        n, i = div(q, I), rem(q, I)
        return pltpu.make_async_copy(
            a.at[n, pl.ds(k * KC, KC), pl.ds(whole_of(i * BM, 128), BM)], abuf.at[k], asem.at[k])

    def gcopy(p, k):
        n, _, col = start(p)
        return pltpu.make_async_copy(
            g.at[n, pl.ds(k * KC, KC), pl.ds(whole_of(col, 128), BN)], gbuf.at[k], gsem.at[k])

    KF = KC // FIRST

    def afirst(k, f):
        rows = pl.ds(k * KC + f * KF, KF)
        return pltpu.make_async_copy(
            a.at[0, rows, pl.ds(0, BM)], abuf.at[k, pl.ds(f * KF, KF)], asem.at[k + f * KS])

    def gfirst(k, f):
        rows = pl.ds(k * KC + f * KF, KF)
        return pltpu.make_async_copy(
            g.at[0, rows, pl.ds(0, BN)], gbuf.at[k, pl.ds(f * KF, KF)], gsem.at[k + f * KS])

    for k in range(KS):
        for f in range(FIRST):
            afirst(k, f).start()
            gfirst(k, f).start()

    def remote(src, dst, s, r, who):
        return pltpu.make_async_remote_copy(src, dst, s, r, device_id=who, device_id_type=MESH)

    class Piece:
        def __init__(self, p, sure, place=None):
            self.p, self.sure, self.place = p, sure, place or start(p)

        def slot(self, n):
            return rem(self.p, n)

        def half(self, core):
            n, row, col = self.place
            row = row + core * HALF
            return out.at[n, pl.ds(whole_of(row, 16), HALF), pl.ds(whole_of(col, 128), BN)]

        def block(self, core, q):
            n, row, col = self.place
            row = row + core * HALF + 2 * q * CH
            return out.at[n, pl.ds(whole_of(row, 16), 2 * CH), pl.ds(whole_of(col, 128), BN)]

        def message(self, q, h):
            n, row, col = self.place
            row, col = row + c * HALF + (2 * q + h // WC) * CH, col + h % WC * CW
            return out.at[n, pl.ds(whole_of(row, 16), CH), pl.ds(whole_of(col, 128), CW)]

        def d_copy(self):
            s = self.slot(ND)
            return remote(dout.at[s], din.at[s], d_s.at[s], d_r.at[s], mate)

        def l_copy(self, h, q):
            s = self.slot(NS)
            return remote(lsend.at[s, h, q], lrecv.at[s, h, q], l_s.at[s], l_r.at[s, h, q], near)

        def p_copy(self, h):
            s = self.slot(NR)
            return remote(psend.at[s, h], precv.at[s, h], p_s.at[s], p_r.at[s, h], peer)

        def t_peer(self, h, q):
            at = self.message(q, h)
            return remote(at, at, t_sp.at[self.slot(NF)], pt_r.at[self.slot(RP), h], peer)

        def t_leaf(self, h, q):
            at = self.message(q, h)
            return remote(at, at, t_sl.at[self.slot(NF)], lt_r.at[self.slot(RL), 0], near)

        def f_leaf(self, h, q):
            at = self.message(q, h)
            return remote(at, at, f_sl.at[self.slot(NF)], lt_r.at[self.slot(RL), 1], near)

        def m_copy(self, q):
            at = self.block(c, q)
            return remote(at, at, m_s.at[self.slot(2)], m_r.at[self.slot(RM)], mate)

        def l_sent(self):
            s = self.slot(NS)
            remote(lsend.at[s], lrecv.at[s], l_s.at[s], l_r.at[s, 0, 0], near).wait_send()

        def p_sent(self):
            s = self.slot(NR)
            remote(psend.at[s], precv.at[s], p_s.at[s], p_r.at[s, 0], peer).wait_send()

        def t_sent(self):
            s, at = self.slot(NF), self.block(c, rq)
            remote(at, at, t_sp.at[s], pt_r.at[0, 0], peer).wait_send()
            remote(at, at, t_sl.at[s], lt_r.at[0, 0], near).wait_send()

        def f_sent(self):
            at = self.block(c, sq)
            remote(at, at, f_sl.at[self.slot(NF)], lt_r.at[0, 0], near).wait_send()

        def m_sent(self):
            at = self.half(c)
            remote(at, at, m_s.at[self.slot(2)], m_r.at[0], mate).wait_send()

        def whole(self, k, q):
            at = self.block(c, q)
            remote(at, at, t_sl.at[0], lt_r.at[self.slot(RL), k], near).wait_recv()

        def given(self):
            at = self.half(1 - c)
            remote(at, at, m_s.at[0], m_r.at[self.slot(RM)], mate).wait_recv()

    def multiply(p, k):
        q, j = div(p, J), rem(p, J)

        @pl.when(j == 0)
        def _():
            acopy(q, k).wait()

        gcopy(p, k).wait()
        d = lax.dot_general(abuf[k], gbuf[k], (((0,), (0,)), ((), ())), preferred_element_type=f32)
        if k == 0:
            acc[...] = d
        else:
            acc[...] += d

        @pl.when(p + 1 < total)
        def _():
            gcopy(p + 1, k).start()

            @pl.when(j == J - 1)
            def _():
                acopy(q + 1, k).start()

    def again(it, n, f):
        if it.sure:
            f()
        else:
            pl.when(it.p >= n)(f)

    def swap(it):
        s, ps = it.slot(ND), it.slot(NP)

        def free():
            it.d_copy().wait_send()
            pl.semaphore_wait(cr_d, 1)
        again(it, ND, free)

        def part(core, h, q):
            rows = pl.ds(pl.multiple_of(core * HALF + (2 * q + h // WC) * CH, 16), CH)
            return acc[rows, h % WC * CW:(h % WC + 1) * CW]

        for h in range(U):
            for q in range(2):
                dout[s, h, q] = part(1 - c, h, q).astype(bf16)
        it.d_copy().start()
        for h in range(U):
            for q in range(2):
                pend[ps, h, q] = part(c, h, q)

    def chip_sum(it):
        it.d_copy().wait_recv()
        ps, ds, ls = it.slot(NP), it.slot(ND), it.slot(NS)

        @pl.when(leaf)
        def _():
            def free():
                pl.semaphore_wait(cr_l, 1)
                it.l_sent()
            again(it, NS, free)
            for h in range(U):
                for q in (sq, rq):
                    lsend[ls, h, q] = (pend[ps, h, q] + din[ds, h, q].astype(f32)).astype(bf16)
                    it.l_copy(h, q).start()

        @pl.when(inner)
        def _():
            for h in range(U):
                for q in range(2):
                    pend[ps, h, q] = pend[ps, h, q] + din[ds, h, q].astype(f32)

        pl.semaphore_signal(cr_d, inc=1, device_id=mate, device_id_type=MESH)

    def forward_partial(it, h):
        it.l_copy(h, sq).wait_recv()
        if h == 0:
            again(it, NR, it.p_sent)
        again(it, NR, lambda: pl.semaphore_wait(cr_p, 1))
        psend[it.slot(NR), h] = (pend[it.slot(NP), h, sq] + lrecv[it.slot(NS), h, sq].astype(f32)).astype(bf16)
        it.p_copy(h).start()

    def finish(it, h):
        it.l_copy(h, rq).wait_recv()
        it.p_copy(h).wait_recv()
        if h == 0:
            again(it, NF, it.t_sent)
        where = it.message(rq, h)
        where[...] = (pend[it.slot(NP), h, rq] + lrecv[it.slot(NS), h, rq].astype(f32)
                      + precv[it.slot(NR), h].astype(f32)).astype(bf16)
        it.t_leaf(h, rq).start()
        it.t_peer(h, rq).start()
        pl.semaphore_signal(cr_p, inc=1, device_id=peer, device_id_type=MESH)
        if h == U - 1:
            again(it, 2, it.m_sent)
            it.m_copy(rq).start()
            pl.semaphore_signal(cr_l, inc=1, device_id=near, device_id_type=MESH)

    def pass_on(it, h):
        it.t_peer(h, sq).wait_recv()
        if h == 0:
            again(it, NF, it.f_sent)
        it.f_leaf(h, sq).start()
        if h == U - 1:
            it.m_copy(sq).start()

    def pass_leaf(it):
        it.whole(0, rq)
        again(it, 2, it.m_sent)
        it.m_copy(rq).start()
        it.whole(1, sq)
        it.m_copy(sq).start()

    def arrived(it):
        it.given()

    def events(pieces, k, phase):
        def due(lag, f, *h):
            if (k - lag) % 4:
                return
            it = pieces[(lag - k) // 4]
            if phase == "body":
                f(it, *h)
            elif phase == "head" or phase == "tail":
                pl.when(it.p >= 0 if phase == "head" else it.p < total)(lambda: f(it, *h))

        def inners(side):
            for lags, f in ((PARTIAL, forward_partial), (FINISH, finish), (PASS, pass_on)):
                for h in range(U):
                    due(lags[side] + 4 // U * h, f, h)

        for side in range(2):
            pl.when(inner & (sd == side))(functools.partial(inners, side))
        due(SUM, chip_sum)

        @pl.when(leaf)
        def _():
            due(LEAF, pass_leaf)

        due(HELD, arrived)

    def recent(p, phase):
        return [Piece(p - n, phase != "head") for n in range(HELD // 4 + 1)]

    def step(phase, p, _):
        pieces = recent(p, phase)
        for k in range(KS):
            multiply(p, k)
            if k == KS - 1:
                swap(pieces[0])
            events(pieces, k, phase)
        return 0

    for k in range(KS):
        for f in range(FIRST):
            afirst(k, f).wait()
            gfirst(k, f).wait()
            rows = slice(f * KF, (f + 1) * KF)
            d = lax.dot_general(
                abuf[k, rows], gbuf[k, rows], (((0,), (0,)), ((), ())), preferred_element_type=f32)
            if k + f == 0:
                acc[...] = d
            else:
                acc[...] += d
        gcopy(1, k).start()
    pl.semaphore_wait(bar, jnp.where(leaf, 2, 3))
    swap(Piece(0, False))

    lax.fori_loop(1, HEAD, functools.partial(step, "head"), 0)
    lax.fori_loop(HEAD, total, functools.partial(step, "body"), 0)

    def tail(p, _):
        pieces = recent(p, "tail")
        for k in range(KS):
            events(pieces, k, "tail")
        return 0

    last = total + HELD // 4 + 1
    lax.fori_loop(total, last - 2, tail, 0)

    def gone(n, f):
        def body(p, _):
            f(Piece(p, True))
            return 0
        lax.fori_loop(total - n, total, body, 0)

    pl.semaphore_wait(cr_d, ND)
    gone(ND, lambda it: it.d_copy().wait_send())

    @pl.when(leaf)
    def _():
        pl.semaphore_wait(cr_l, NS)
        gone(NS, Piece.l_sent)

    @pl.when(inner)
    def _():
        pl.semaphore_wait(cr_p, NR * U)
        gone(NR, Piece.p_sent)
        gone(NF, Piece.t_sent)
        gone(NF, Piece.f_sent)

    lax.fori_loop(last - 2, last, tail, 0)

    gone(2, Piece.m_sent)


def put(x, out, sems):
    rows = x.shape[1] // PUT
    copies = [
        pltpu.make_async_copy(x.at[n, pl.ds(r * rows, rows)], out.at[n, pl.ds(r * rows, rows)], sems.at[n, r])
        for n in range(x.shape[0]) for r in range(PUT)
    ]
    for one in copies:
        one.start()
    for one in copies:
        one.wait()


def solution(mesh):
    def step(a, g):
        _, nm, K, M = a.shape
        N = g.shape[-1]
        a, g = a.reshape(nm, K, M), g.reshape(nm, K, N)
        dma = pltpu.SemaphoreType.DMA
        bf16, f32 = jnp.bfloat16, jnp.float32
        sums = pl.pallas_call(
            functools.partial(kernel, (nm, K, M, N)),
            out_shape=pltpu.VMEM((nm, M, N), bf16),
            in_specs=[pl.BlockSpec(memory_space=pl.ANY)] * 2,
            out_specs=pl.BlockSpec(memory_space=pltpu.VMEM),
            scratch_shapes=[
                pltpu.VMEM((KS, K // KS, BM), bf16),
                pltpu.VMEM((KS, K // KS, BN), bf16),
                pltpu.VMEM((BM, BN), f32),
                pltpu.VMEM((NP, U, 2, CH, CW), f32),
                pltpu.VMEM((ND, U, 2, CH, CW), bf16),
                pltpu.VMEM((ND, U, 2, CH, CW), bf16),
                pltpu.VMEM((NS, U, 2, CH, CW), bf16),
                pltpu.VMEM((NS, U, 2, CH, CW), bf16),
                pltpu.VMEM((NR, U, CH, CW), bf16),
                pltpu.VMEM((NR, U, CH, CW), bf16),
                dma((KS * FIRST,)), dma((KS * FIRST,)), dma((ND,)), dma((ND,)), dma((NS,)), dma((NS, U, 2)),
                dma((NR,)), dma((NR, U)), dma((NF,)), dma((NF,)), dma((NF,)), dma((2,)),
                dma((RP, U)), dma((RL, 2)), dma((RM,)),
                pltpu.SemaphoreType.REGULAR, pltpu.SemaphoreType.REGULAR, pltpu.SemaphoreType.REGULAR,
            ],
            compiler_params=pltpu.CompilerParams(
                collective_id=0, has_side_effects=True, vmem_limit_bytes=33 * 2**20
            ),
        )(a, g)
        return pl.pallas_call(
            put,
            out_shape=jax.ShapeDtypeStruct((nm, M, N), bf16),
            in_specs=[pl.BlockSpec(memory_space=pltpu.VMEM)],
            out_specs=pl.BlockSpec(memory_space=pl.ANY),
            scratch_shapes=[dma((nm, PUT))],
            compiler_params=pltpu.CompilerParams(vmem_limit_bytes=2**20),
        )(sums)

    return jax.shard_map(
        step,
        mesh=mesh,
        in_specs=(P(("rep", "dp"), None, None, None),) * 2,
        out_specs=P("rep", None, None),
        check_vma=False,
    )
```

```python
import functools

import jax
import jax.numpy as jnp
from jax import lax
from jax.experimental import pallas as pl
from jax.experimental.pallas import tpu as pltpu
from jax.sharding import PartitionSpec as P

MESH = pl.DeviceIdType.MESH
BM, BN, KS = 640, 512, 4
FIRST = 2
U = 2
HALF, CH, CW = BM // 2, BM // 8, 2 * BN // U
WC = BN // CW
ND, NP, NS, NR, NF = 2, 4, 3, 2, 2
RP, RL, RM = 2, 4, 7
SUM, HELD = 4, 25
PARTIAL = 5, 5
FINISH = 9, 6
PASS = 10, 11
LEAF = 19
HEAD = 10
PUT = 4


def div(x, n):
    return x // n if isinstance(x, int) else lax.div(x, n)


def rem(x, n):
    return x % n if isinstance(x, int) else lax.rem(x, n)


def whole_of(x, n):
    return x if isinstance(x, int) else pl.multiple_of(x, n)


def kernel(dims, a, g, out, abuf, gbuf, acc, pend, dout, din, lsend, lrecv, psend, precv,
           asem, gsem, d_s, d_r, l_s, l_r, p_s, p_r, t_sp, t_sl, f_sl, m_s, pt_r, lt_r, m_r,
           cr_d, cr_l, cr_p):
    nm, K, M, N = dims
    I, J, KC = M // BM, N // BN, K // KS
    total = nm * I * J
    rep, dp = lax.axis_index("rep"), lax.axis_index("dp")
    z, c = lax.div(dp, 2), lax.rem(dp, 2)
    sd = lax.div(z, 2)
    leaf = (z == 0) | (z == 3)
    inner = jnp.logical_not(leaf)
    rq, sq = sd, 1 - sd
    mate = (rep, z * 2 + 1 - c)
    near = (rep, jnp.where(leaf, 1 + sd, 3 * sd) * 2 + 1 - c)
    peer = (rep, (2 - sd) * 2 + 1 - c)
    own = lax.rem(c + z, 2)
    f32, bf16 = jnp.float32, jnp.bfloat16

    def start(p):
        n, i, j = div(p, I * J), rem(div(p, J), I), rem(p, J)
        return n, i * BM, j * BN

    def acopy(q, k):
        n, i = div(q, I), rem(q, I)
        return pltpu.make_async_copy(
            a.at[n, pl.ds(k * KC, KC), pl.ds(whole_of(i * BM, 128), BM)], abuf.at[k], asem.at[k])

    def gcopy(p, k):
        n, _, col = start(p)
        return pltpu.make_async_copy(
            g.at[n, pl.ds(k * KC, KC), pl.ds(whole_of(col, 128), BN)], gbuf.at[k], gsem.at[k])

    KF = KC // FIRST

    def afirst(k, f):
        rows = pl.ds(k * KC + f * KF, KF)
        return pltpu.make_async_copy(
            a.at[0, rows, pl.ds(0, BM)], abuf.at[k, pl.ds(f * KF, KF)], asem.at[k + f * KS])

    def gfirst(k, f):
        rows = pl.ds(k * KC + f * KF, KF)
        return pltpu.make_async_copy(
            g.at[0, rows, pl.ds(0, BN)], gbuf.at[k, pl.ds(f * KF, KF)], gsem.at[k + f * KS])

    for k in range(KS):
        for f in range(FIRST):
            afirst(k, f).start()
            gfirst(k, f).start()

    bar = pltpu.get_barrier_semaphore()
    pl.semaphore_signal(bar, inc=1, device_id=mate, device_id_type=MESH)
    pl.semaphore_signal(bar, inc=1, device_id=near, device_id_type=MESH)

    @pl.when(inner)
    def _():
        pl.semaphore_signal(bar, inc=1, device_id=peer, device_id_type=MESH)

    def remote(src, dst, s, r, who):
        return pltpu.make_async_remote_copy(src, dst, s, r, device_id=who, device_id_type=MESH)

    class Piece:
        def __init__(self, p, sure, place=None):
            self.p, self.sure, self.place = p, sure, place or start(p)

        def slot(self, n):
            return rem(self.p, n)

        def half(self, core):
            n, row, col = self.place
            row = row + core * HALF
            return out.at[n, pl.ds(whole_of(row, 16), HALF), pl.ds(whole_of(col, 128), BN)]

        def block(self, core, q):
            n, row, col = self.place
            row = row + core * HALF + 2 * q * CH
            return out.at[n, pl.ds(whole_of(row, 16), 2 * CH), pl.ds(whole_of(col, 128), BN)]

        def message(self, q, h):
            n, row, col = self.place
            row, col = row + own * HALF + (2 * q + h // WC) * CH, col + h % WC * CW
            return out.at[n, pl.ds(whole_of(row, 16), CH), pl.ds(whole_of(col, 128), CW)]

        def d_copy(self):
            s = self.slot(ND)
            return remote(dout.at[s], din.at[s], d_s.at[s], d_r.at[s], mate)

        def l_copy(self, h, q):
            s = self.slot(NS)
            return remote(lsend.at[s, h, q], lrecv.at[s, h, q], l_s.at[s], l_r.at[s, h, q], near)

        def p_copy(self, h):
            s = self.slot(NR)
            return remote(psend.at[s, h], precv.at[s, h], p_s.at[s], p_r.at[s, h], peer)

        def t_peer(self, h, q):
            at = self.message(q, h)
            return remote(at, at, t_sp.at[self.slot(NF)], pt_r.at[self.slot(RP), h], peer)

        def t_leaf(self, h, q):
            at = self.message(q, h)
            return remote(at, at, t_sl.at[self.slot(NF)], lt_r.at[self.slot(RL), 0], near)

        def f_leaf(self, h, q):
            at = self.message(q, h)
            return remote(at, at, f_sl.at[self.slot(NF)], lt_r.at[self.slot(RL), 1], near)

        def m_copy(self, q):
            at = self.block(own, q)
            return remote(at, at, m_s.at[self.slot(2)], m_r.at[self.slot(RM)], mate)

        def l_sent(self):
            s = self.slot(NS)
            remote(lsend.at[s], lrecv.at[s], l_s.at[s], l_r.at[s, 0, 0], near).wait_send()

        def p_sent(self):
            s = self.slot(NR)
            remote(psend.at[s], precv.at[s], p_s.at[s], p_r.at[s, 0], peer).wait_send()

        def t_sent(self):
            s, at = self.slot(NF), self.block(own, rq)
            remote(at, at, t_sp.at[s], pt_r.at[0, 0], peer).wait_send()
            remote(at, at, t_sl.at[s], lt_r.at[0, 0], near).wait_send()

        def f_sent(self):
            at = self.block(own, sq)
            remote(at, at, f_sl.at[self.slot(NF)], lt_r.at[0, 0], near).wait_send()

        def m_sent(self):
            at = self.half(own)
            remote(at, at, m_s.at[self.slot(2)], m_r.at[0], mate).wait_send()

        def whole(self, k, q):
            at = self.block(own, q)
            remote(at, at, t_sl.at[0], lt_r.at[self.slot(RL), k], near).wait_recv()

        def given(self):
            at = self.half(1 - own)
            remote(at, at, m_s.at[0], m_r.at[self.slot(RM)], mate).wait_recv()

    def multiply(p, k):
        q, j = div(p, J), rem(p, J)

        @pl.when(j == 0)
        def _():
            acopy(q, k).wait()

        gcopy(p, k).wait()
        d = lax.dot_general(abuf[k], gbuf[k], (((0,), (0,)), ((), ())), preferred_element_type=f32)
        if k == 0:
            acc[...] = d
        else:
            acc[...] += d

        @pl.when(p + 1 < total)
        def _():
            gcopy(p + 1, k).start()

            @pl.when(j == J - 1)
            def _():
                acopy(q + 1, k).start()

    def again(it, n, f):
        if it.sure:
            f()
        else:
            pl.when(it.p >= n)(f)

    def swap(it):
        s, ps = it.slot(ND), it.slot(NP)

        def free():
            it.d_copy().wait_send()
            pl.semaphore_wait(cr_d, 1)
        again(it, ND, free)

        def part(core, h, q):
            rows = pl.ds(pl.multiple_of(core * HALF + (2 * q + h // WC) * CH, 16), CH)
            return acc[rows, h % WC * CW:(h % WC + 1) * CW]

        for h in range(U):
            for q in range(2):
                dout[s, h, q] = part(1 - own, h, q).astype(bf16)
        it.d_copy().start()
        for h in range(U):
            for q in range(2):
                pend[ps, h, q] = part(own, h, q)

    def chip_sum(it):
        it.d_copy().wait_recv()
        ps, ds, ls = it.slot(NP), it.slot(ND), it.slot(NS)

        @pl.when(leaf)
        def _():
            def free():
                pl.semaphore_wait(cr_l, 1)
                it.l_sent()
            again(it, NS, free)
            for h in range(U):
                for q in (sq, rq):
                    lsend[ls, h, q] = (pend[ps, h, q] + din[ds, h, q].astype(f32)).astype(bf16)
                    it.l_copy(h, q).start()

        @pl.when(inner)
        def _():
            for h in range(U):
                for q in range(2):
                    pend[ps, h, q] = pend[ps, h, q] + din[ds, h, q].astype(f32)

        pl.semaphore_signal(cr_d, inc=1, device_id=mate, device_id_type=MESH)

    def forward_partial(it, h):
        it.l_copy(h, sq).wait_recv()
        if h == 0:
            again(it, NR, it.p_sent)
        again(it, NR, lambda: pl.semaphore_wait(cr_p, 1))
        psend[it.slot(NR), h] = (pend[it.slot(NP), h, sq] + lrecv[it.slot(NS), h, sq].astype(f32)).astype(bf16)
        it.p_copy(h).start()

    def finish(it, h):
        it.l_copy(h, rq).wait_recv()
        it.p_copy(h).wait_recv()
        if h == 0:
            again(it, NF, it.t_sent)
        where = it.message(rq, h)
        where[...] = (pend[it.slot(NP), h, rq] + lrecv[it.slot(NS), h, rq].astype(f32)
                      + precv[it.slot(NR), h].astype(f32)).astype(bf16)
        it.t_leaf(h, rq).start()
        it.t_peer(h, rq).start()
        pl.semaphore_signal(cr_p, inc=1, device_id=peer, device_id_type=MESH)
        if h == U - 1:
            again(it, 2, it.m_sent)
            it.m_copy(rq).start()
            pl.semaphore_signal(cr_l, inc=1, device_id=near, device_id_type=MESH)

    def pass_on(it, h):
        it.t_peer(h, sq).wait_recv()
        if h == 0:
            again(it, NF, it.f_sent)
        it.f_leaf(h, sq).start()
        if h == U - 1:
            it.m_copy(sq).start()

    def pass_leaf(it):
        it.whole(0, rq)
        again(it, 2, it.m_sent)
        it.m_copy(rq).start()
        it.whole(1, sq)
        it.m_copy(sq).start()

    def arrived(it):
        it.given()

    def events(pieces, k, phase):
        def due(lag, f, *h):
            if (k - lag) % 4:
                return
            it = pieces[(lag - k) // 4]
            if phase == "body":
                f(it, *h)
            elif phase == "head" or phase == "tail":
                pl.when(it.p >= 0 if phase == "head" else it.p < total)(lambda: f(it, *h))

        def inners(side):
            for lags, f in ((PARTIAL, forward_partial), (FINISH, finish), (PASS, pass_on)):
                for h in range(U):
                    due(lags[side] + 4 // U * h, f, h)

        for side in range(2):
            pl.when(inner & (sd == side))(functools.partial(inners, side))
        due(SUM, chip_sum)

        @pl.when(leaf)
        def _():
            due(LEAF, pass_leaf)

        due(HELD, arrived)

    def recent(p, phase):
        return [Piece(p - n, phase != "head") for n in range(HELD // 4 + 1)]

    def step(phase, p, _):
        pieces = recent(p, phase)
        for k in range(KS):
            multiply(p, k)
            if k == KS - 1:
                swap(pieces[0])
            events(pieces, k, phase)
        return 0

    for k in range(KS):
        for f in range(FIRST):
            afirst(k, f).wait()
            gfirst(k, f).wait()
            rows = slice(f * KF, (f + 1) * KF)
            d = lax.dot_general(
                abuf[k, rows], gbuf[k, rows], (((0,), (0,)), ((), ())), preferred_element_type=f32)
            if k + f == 0:
                acc[...] = d
            else:
                acc[...] += d
        gcopy(1, k).start()
    pl.semaphore_wait(bar, jnp.where(leaf, 2, 3))
    swap(Piece(0, False))
    step("head", 1, 0)

    lax.fori_loop(2, HEAD, functools.partial(step, "head"), 0)
    lax.fori_loop(HEAD, total, functools.partial(step, "body"), 0)

    def tail(p, _):
        pieces = recent(p, "tail")
        for k in range(KS):
            events(pieces, k, "tail")
        return 0

    last = total + HELD // 4 + 1
    lax.fori_loop(total, last - 2, tail, 0)

    def gone(n, f):
        def body(p, _):
            f(Piece(p, True))
            return 0
        lax.fori_loop(total - n, total, body, 0)

    pl.semaphore_wait(cr_d, ND)
    gone(ND, lambda it: it.d_copy().wait_send())

    @pl.when(leaf)
    def _():
        pl.semaphore_wait(cr_l, NS)
        gone(NS, Piece.l_sent)

    @pl.when(inner)
    def _():
        pl.semaphore_wait(cr_p, NR * U)
        gone(NR, Piece.p_sent)
        gone(NF, Piece.t_sent)
        gone(NF, Piece.f_sent)

    lax.fori_loop(last - 2, last, tail, 0)

    gone(2, Piece.m_sent)


def put(x, out, sems):
    rows = x.shape[1] // PUT
    copies = [
        pltpu.make_async_copy(x.at[n, pl.ds(r * rows, rows)], out.at[n, pl.ds(r * rows, rows)], sems.at[n, r])
        for n in range(x.shape[0]) for r in range(PUT)
    ]
    for one in copies:
        one.start()
    for one in copies:
        one.wait()


def solution(mesh):
    def step(a, g):
        _, nm, K, M = a.shape
        N = g.shape[-1]
        a, g = a.reshape(nm, K, M), g.reshape(nm, K, N)
        dma = pltpu.SemaphoreType.DMA
        bf16, f32 = jnp.bfloat16, jnp.float32
        sums = pl.pallas_call(
            functools.partial(kernel, (nm, K, M, N)),
            out_shape=pltpu.VMEM((nm, M, N), bf16),
            in_specs=[pl.BlockSpec(memory_space=pl.ANY)] * 2,
            out_specs=pl.BlockSpec(memory_space=pltpu.VMEM),
            scratch_shapes=[
                pltpu.VMEM((KS, K // KS, BM), bf16),
                pltpu.VMEM((KS, K // KS, BN), bf16),
                pltpu.VMEM((BM, BN), f32),
                pltpu.VMEM((NP, U, 2, CH, CW), f32),
                pltpu.VMEM((ND, U, 2, CH, CW), bf16),
                pltpu.VMEM((ND, U, 2, CH, CW), bf16),
                pltpu.VMEM((NS, U, 2, CH, CW), bf16),
                pltpu.VMEM((NS, U, 2, CH, CW), bf16),
                pltpu.VMEM((NR, U, CH, CW), bf16),
                pltpu.VMEM((NR, U, CH, CW), bf16),
                dma((KS * FIRST,)), dma((KS * FIRST,)), dma((ND,)), dma((ND,)), dma((NS,)), dma((NS, U, 2)),
                dma((NR,)), dma((NR, U)), dma((NF,)), dma((NF,)), dma((NF,)), dma((2,)),
                dma((RP, U)), dma((RL, 2)), dma((RM,)),
                pltpu.SemaphoreType.REGULAR, pltpu.SemaphoreType.REGULAR, pltpu.SemaphoreType.REGULAR,
            ],
            compiler_params=pltpu.CompilerParams(
                collective_id=0, has_side_effects=True, vmem_limit_bytes=33 * 2**20
            ),
        )(a, g)
        return pl.pallas_call(
            put,
            out_shape=jax.ShapeDtypeStruct((nm, M, N), bf16),
            in_specs=[pl.BlockSpec(memory_space=pltpu.VMEM)],
            out_specs=pl.BlockSpec(memory_space=pl.ANY),
            scratch_shapes=[dma((nm, PUT))],
            compiler_params=pltpu.CompilerParams(vmem_limit_bytes=2**20),
        )(sums)

    return jax.shard_map(
        step,
        mesh=mesh,
        in_specs=(P(("rep", "dp"), None, None, None),) * 2,
        out_specs=P("rep", None, None),
        check_vma=False,
    )
```
